32 devices in a mesh: gx: 4 (over y, x), gy: 8 (over z, core).
Axes of the slice: x: 2, y: 2, z: 4, core: 2. Of those that a mesh axis runs over, the one named last changes fastest.
Arguments:
- value_field: float32 [4, 24, 48, 1536], P(None, 'gx', 'gy'), may hold values from -16 to 17
- target_mask: int32 [4, 24, 48, 1536], P(None, 'gx', 'gy'), may hold values 0 or 1
- obstacle_mask: int32 [4, 24, 48, 1536], P(None, 'gx', 'gy'), may hold values 0 or 1
- drift_gains: float32 [5], replicated, may hold values from 0.5 to 2
- control_costs: float32 [5], replicated, may hold values from 0.25 to 1
Outputs:
- reach_value: float32 [4, 24, 48, 1536], P(None, 'gx', 'gy')
- time_steps: float32 [3], replicated
The draws below stay inside these ranges and needn't reach their ends.
All inputs are finite; a program needn't handle non-finite values. No bound on the sum of `target_mask` or of `obstacle_mask` on one device may be relied on, other than what follows from the above.
Results may differ from the reference program's by a relative error of at most 0.0003.
Values sent between devices are 32-bit elements; how exact they have to be, the bound alone decides.
A program may use at most 128 MiB of HBM per device.

```python
import math
import jax
import jax.numpy as jnp
from jax import lax

PLANES = 4
N3 = 32
N4 = 48
GRID = 96
STEPS = 3
NA = 24
NB = 48


def draw_value_field(key, part):
    base_key = jax.random.fold_in(key, 11)
    rough_key, row_key, col_key = jax.random.split(base_key, 3)
    grid_shape = (PLANES, NA, NB, N3 * N4)
    rough_part = jnp.clip(jax.random.normal(rough_key, grid_shape, jnp.float32), -4.0, 4.0)
    row_scale = jnp.exp(jax.random.uniform(row_key, (NA,), jnp.float32, -math.log(2.0), math.log(2.0)))
    col_scale = jnp.exp(jax.random.uniform(col_key, (NB,), jnp.float32, -math.log(2.0), math.log(2.0)))
    return rough_part * row_scale[None, :, None, None] * col_scale[None, None, :, None]


def with_ends(values, own_key, smallest, largest):
    place = [jax.random.randint(jax.random.fold_in(own_key, axis), (), 0, length) for axis, length in enumerate(values.shape)]
    main_axis = values.shape.index(max(values.shape))
    neighbour = place[:main_axis] + [(place[main_axis] + 1) % values.shape[main_axis]] + place[main_axis + 1:]
    return values.at[tuple(place)].set(smallest).at[tuple(neighbour)].set(largest)


def setup_inputs(seed: int = 0) -> dict:
    splits = jax.random.split(jax.random.key(seed), 6)
    return {
        "value_field": draw_value_field(jax.random.fold_in(splits[5], 71), 0),
        "target_mask": with_ends((jax.random.randint(splits[1], (PLANES, NA, NB, N3 * N4), 0, 4) < 1).astype(jnp.int32), jax.random.fold_in(splits[1], 1), 0, 1),
        "obstacle_mask": with_ends((jax.random.randint(splits[2], (PLANES, NA, NB, N3 * N4), 0, 5) < 1).astype(jnp.int32), jax.random.fold_in(splits[2], 1), 0, 1),
        "drift_gains": jnp.clip(jnp.exp(jax.random.uniform(splits[3], (5,), jnp.float32, math.log(0.5), math.log(2.0))), 0.5, 2.0),
        "control_costs": jnp.clip(jnp.exp(jax.random.uniform(splits[4], (5,), jnp.float32, math.log(0.25), math.log(1.0))), 0.25, 1.0),
    }


courant = 0.5
weno_eps = 1e-6


def weno_side(diff_one, diff_two, diff_three, diff_four, diff_five):
    stencil_one = diff_one / 3.0 - 7.0 * diff_two / 6.0 + 11.0 * diff_three / 6.0
    stencil_two = -diff_two / 6.0 + 5.0 * diff_three / 6.0 + diff_four / 3.0
    stencil_three = diff_three / 3.0 + 5.0 * diff_four / 6.0 - diff_five / 6.0
    smooth_one = 13.0 / 12.0 * (diff_one - 2.0 * diff_two + diff_three) ** 2 + 0.25 * (diff_one - 4.0 * diff_two + 3.0 * diff_three) ** 2
    smooth_two = 13.0 / 12.0 * (diff_two - 2.0 * diff_three + diff_four) ** 2 + 0.25 * (diff_two - diff_four) ** 2
    smooth_three = 13.0 / 12.0 * (diff_three - 2.0 * diff_four + diff_five) ** 2 + 0.25 * (3.0 * diff_three - 4.0 * diff_four + diff_five) ** 2
    weight_one = 0.1 / (weno_eps + smooth_one) ** 2
    weight_two = 0.6 / (weno_eps + smooth_two) ** 2
    weight_three = 0.3 / (weno_eps + smooth_three) ** 2
    return (weight_one * stencil_one + weight_two * stencil_two + weight_three * stencil_three) / (weight_one + weight_two + weight_three)


def axis_slopes(shifted, spacing):
    differences = [shifted[offset + 1] - shifted[offset] for offset in range(6)]
    minus_slope = weno_side(differences[0], differences[1], differences[2], differences[3], differences[4]) / spacing
    plus_slope = weno_side(differences[5], differences[4], differences[3], differences[2], differences[1]) / spacing
    return minus_slope, plus_slope


def merged_shifts(interior, stride, position, extent):
    upward = []
    current = interior
    for offset in range(1, 4):
        current = jnp.where(position + offset <= extent - 1, jnp.roll(interior, -offset * stride, axis=-1), current)
        upward.append(current)
    downward = []
    current = interior
    for offset in range(1, 4):
        current = jnp.where(position - offset >= 0, jnp.roll(interior, offset * stride, axis=-1), current)
        downward.append(current)
    return [downward[2], downward[1], downward[0], interior, upward[0], upward[1], upward[2]]


def drift_field(first_pos, heading_one, heading_two, third_pos, fourth_pos, drift_gains):
    return [drift_gains[0] * (jnp.cos(heading_one) - 0.5 * jnp.cos(heading_two) + third_pos),
            drift_gains[1] * (fourth_pos - 0.3 * first_pos),
            drift_gains[2] * (third_pos + 0.5 * jnp.sin(heading_one)),
            drift_gains[3] * (jnp.sin(heading_two) - first_pos),
            drift_gains[4] * (jnp.cos(heading_one) * jnp.sin(heading_two) - fourth_pos)]


def local_bounds(drift_terms, slopes, control_costs, spacing_list):
    peaks = []
    for axis_number in range(5):
        scale = control_costs[axis_number] * spacing_list[axis_number]
        minus_peak = jnp.max(jnp.abs(drift_terms[axis_number] - scale * slopes[axis_number][0]))
        plus_peak = jnp.max(jnp.abs(drift_terms[axis_number] - scale * slopes[axis_number][1]))
        peaks.append(jnp.maximum(minus_peak, plus_peak))
    return jnp.stack(peaks)


def advance(interior, slopes, drift_terms, bounds, time_step, control_costs, spacing_list, target_plane, obstacle_plane):
    hamiltonian = jnp.zeros_like(interior)
    for axis_number in range(5):
        minus_slope, plus_slope = slopes[axis_number]
        middle = 0.5 * (minus_slope + plus_slope)
        hamiltonian = hamiltonian + drift_terms[axis_number] * middle - 0.5 * control_costs[axis_number] * spacing_list[axis_number] * middle * middle
        hamiltonian = hamiltonian - bounds[axis_number] * 0.5 * (plus_slope - minus_slope)
    advanced = interior - time_step * hamiltonian
    advanced = jnp.where(target_plane == 1, jnp.minimum(advanced, -0.5), advanced)
    return jnp.where(obstacle_plane == 1, jnp.maximum(advanced, 0.5), advanced)


def plane_state(padded, plane_index, drift_gains, spacing_list):
    center = lax.dynamic_index_in_dim(padded, plane_index, 0, keepdims=False)
    interior = center[3:-3, 3:-3]
    neighbours = [lax.dynamic_index_in_dim(padded, jnp.clip(plane_index + offset - 3, 0, PLANES - 1).astype(jnp.int32), 0, keepdims=False)[3:-3, 3:-3] for offset in range(7)]
    row_shifts = [center[offset:offset + NA, 3:-3] for offset in range(7)]
    col_shifts = [center[3:-3, offset:offset + NB] for offset in range(7)]
    lane_index = jnp.arange(N3 * N4, dtype=jnp.int32)
    slopes = [axis_slopes(neighbours, spacing_list[0]),
              axis_slopes(row_shifts, spacing_list[1]),
              axis_slopes(col_shifts, spacing_list[2]),
              axis_slopes(merged_shifts(interior, N4, lane_index // N4, N3), spacing_list[3]),
              axis_slopes(merged_shifts(interior, 1, lane_index % N4, N4), spacing_list[4])]
    first_pos = (plane_index.astype(jnp.float32) - PLANES / 2 + 0.5) * (2.0 / GRID)
    heading_one = ((2.0 * math.pi / NA) * jnp.arange(NA, dtype=jnp.float32)).reshape(NA, 1, 1)
    heading_two = ((2.0 * math.pi / NB) * jnp.arange(NB, dtype=jnp.float32)).reshape(1, NB, 1)
    third_pos = (((lane_index // N4).astype(jnp.float32) - N3 / 2 + 0.5) * (2.0 / GRID)).reshape(1, 1, -1)
    fourth_pos = (((lane_index % N4).astype(jnp.float32) - N4 / 2 + 0.5) * (2.0 / GRID)).reshape(1, 1, -1)
    drift_terms = drift_field(first_pos, heading_one, heading_two, third_pos, fourth_pos, drift_gains)
    return interior, slopes, drift_terms


def reference(value_field, target_mask, obstacle_mask, drift_gains, control_costs):
    spacing_list = [2.0 / GRID, 2.0 * math.pi / NA, 2.0 * math.pi / NB, 2.0 / GRID, 2.0 / GRID]
    spacing_array = jnp.array(spacing_list, dtype=jnp.float32)
    plane_ids = jnp.arange(PLANES, dtype=jnp.int32)
    value_now = value_field
    step_sizes = []
    for section_number in range(STEPS):
        padded = jnp.pad(value_now, ((0, 0), (3, 3), (3, 3), (0, 0)), mode="wrap")

        def bound_plane(plane_index):
            interior, slopes, drift_terms = plane_state(padded, plane_index, drift_gains, spacing_list)
            return local_bounds(drift_terms, slopes, control_costs, spacing_list)

        bounds = jnp.max(lax.map(bound_plane, plane_ids), axis=0)
        time_step = courant / (jnp.sum(bounds / spacing_array) + 1e-6)

        def move_plane(items):
            plane_index, target_plane, obstacle_plane = items
            interior, slopes, drift_terms = plane_state(padded, plane_index, drift_gains, spacing_list)
            return advance(interior, slopes, drift_terms, bounds, time_step, control_costs, spacing_list, target_plane, obstacle_plane)

        value_now = lax.map(move_plane, (plane_ids, target_mask, obstacle_mask))
        step_sizes.append(time_step)
    return value_now, jnp.stack(step_sizes)
```

```python
import functools
import math

import jax
import jax.numpy as jnp
import numpy as np
from jax import lax
from jax.experimental import pallas as pl
from jax.experimental.pallas import tpu as pltpu
from jax.sharding import PartitionSpec as P

N3 = 32
N4 = 48
GRID = 96
STEPS = 3
COURANT = 0.5
EPS = 0.75e-6
LANES = 128
PAD = 16
MESH = pl.DeviceIdType.MESH


def sub(x, y):
    if x is None or y is None:
        return x if y is None else -y
    return x - y


def add(x, y):
    if x is None or y is None:
        return x if y is None else y
    return x + y


def mul(x, y):
    return None if x is None or y is None else x * y


def wave(d):
    n = len(d) - 5
    f = [sub(d[k + 1], d[k]) for k in range(n + 4)]
    e = [sub(f[k + 1], f[k]) for k in range(n + 3)]
    j = [sub(e[k + 1], e[k]) for k in range(n + 2)]
    g = [mul(0.75, x) for x in f]
    g2 = [add(x, x) for x in g]
    base = [add(add(mul(e[k], e[k]), EPS), mul(g[k], f[k + 1])) for k in range(n + 3)]
    left, mid, right = [], [], []
    for k in range(n + 1):
        a = add(base[k], mul(g2[k + 1], e[k]))
        b = base[k + 1]
        c = sub(base[k + 2], mul(g2[k + 2], e[k + 2]))
        left.append(a * a)
        mid.append(b * b)
        right.append(c * c)
    low, high = [], []
    for k in range(n + 1):
        bc = mid[k] * right[k]
        ab = left[k] * mid[k]
        ac = 6.0 * (left[k] * right[k])
        n1 = mul(bc, j[k])
        n2 = mul(ab, j[k + 1])
        if 0 < k < n:
            both = add(n1, n2)
            both = add(both, both)
            core = (bc + ab) + ac
            low.append(add(both, n2) / (core + (ab + ab)))
            high.append(add(both, n1) / (core + (bc + bc)))
        elif k == 0:
            low.append(add(add(n1, n1), 3.0 * n2) / ((bc + ac) + 3.0 * ab))
            high.append(None)
        else:
            low.append(None)
            high.append(add(add(n2, n2), mul(3.0, n1)) / ((ab + ac) + 3.0 * bc))
    out = []
    for i in range(n):
        rm, rp = low[i], high[i + 1]
        center = mul(6.0, add(d[i + 3], d[i + 2]))
        middle = add(sub(center, add(e[i + 1], e[i + 2])), rp - rm)
        jump = sub(rp + rm, j[i + 1])
        out.append((middle, jump))
    return out


def gaps(vs):
    return [None if a is b else b - a for a, b in zip(vs[:-1], vs[1:])]


def tally(middle, jump, drift, kappa):
    gap = drift - middle
    return jnp.abs(gap) + jnp.abs(jump), (kappa * middle) * (drift + gap)


def kernel(
    dims, sizes,
    cost_ref, gain_ref, trig_ref, v_hbm, t_hbm, o_hbm,
    out_hbm, dt_ref,
    v, t, o, h, q, ra, rb, ca, cb, f0, f1, f2, f3, f4r, f4k, keep, own, slots,
    in_sem, out_sem, rs_sem, rr_sem, cs_sem, cr_sem, ts_sem, tr_sem,
):
    planes, rows, cols, width = dims
    nx, ny = sizes
    chunks = width // LANES
    block = planes * chunks
    parts = block // 8
    pair = 8 // planes
    cells = rows * cols
    ix, iy = lax.axis_index("gx"), lax.axis_index("gy")
    n = nx * ny
    me = ix * ny + iy
    h1 = 2.0 * math.pi / (rows * nx)
    h2 = 2.0 * math.pi / (cols * ny)
    spacing = [2.0 / GRID, h1, h2, 2.0 / GRID, 2.0 / GRID]

    def place(k):
        other = (me + k) % n
        return (other // ny, other % ny)

    def at(c, r):
        return PAD + (c * rows + r) * block

    def span(start, size=8):
        return pl.ds(pl.multiple_of(start, 8), size)

    def loads(c):
        out = []
        for r in range(rows):
            out.append(
                pltpu.make_async_copy(
                    v_hbm.at[r * cols + c],
                    v.at[pl.ds(PAD + (c * rows + r) * block, block)],
                    in_sem.at[c * rows + r],
                )
            )
        return out

    def masks():
        out = []
        for slot, (src, dst) in enumerate(((t_hbm, t), (o_hbm, o))):
            for c in range(cols):
                for r in range(rows):
                    out.append(
                        pltpu.make_async_copy(
                            src.at[r * cols + c],
                            dst.at[pl.ds((c * rows + r) * block, block)],
                            in_sem.at[(slot + 1) * cells + c * rows + r],
                        )
                    )
        return out

    def stores(c):
        out = []
        for r in range(rows):
            out.append(
                pltpu.make_async_copy(
                    v.at[pl.ds(PAD + (c * rows + r) * block, block)],
                    out_hbm.at[r * cols + c],
                    out_sem.at[c * rows + r],
                )
            )
        return out

    tall = 3 * block
    up = ((ix + 1) % nx, iy)
    down = ((ix + nx - 1) % nx, iy)
    after = (ix, (iy + 1) % ny)
    before = (ix, (iy + ny - 1) % ny)

    def row_copy(c, which):
        first = PAD + c * rows * block + (0 if which else (rows - 3) * block)
        return pltpu.make_async_remote_copy(
            src_ref=v.at[pl.ds(first, tall)],
            dst_ref=(rb if which else ra).at[pl.ds(c * tall, tall)],
            send_sem=rs_sem.at[c, which],
            recv_sem=rr_sem.at[c, which],
            device_id=down if which else up,
            device_id_type=MESH,
        )

    def col_copy(c, which):
        wide = rows * block
        i = c if which else c - (cols - 3)
        return pltpu.make_async_remote_copy(
            src_ref=v.at[pl.ds(PAD + c * wide, wide)],
            dst_ref=(cb if which else ca).at[pl.ds(i * wide, wide)],
            send_sem=cs_sem.at[i, which],
            recv_sem=cr_sem.at[i, which],
            device_id=before if which else after,
            device_id_type=MESH,
        )

    def col_copies(c):
        out = []
        if c < 3:
            out.append(col_copy(c, 1))
        if c >= cols - 3:
            out.append(col_copy(c, 0))
        return out

    def sends(c):
        return [row_copy(c, 0), row_copy(c, 1)] + col_copies(c)

    for c in range(cols):
        for copy in loads(c):
            copy.start()
    for copy in masks():
        copy.start()

    barrier = pltpu.get_barrier_semaphore()

    def greet(k, carry):
        pl.semaphore_signal(barrier, inc=1, device_id=place(k), device_id_type=MESH)
        return carry

    lax.fori_loop(1, n, greet, 0)

    full = lambda x: jnp.full((8, LANES), x, jnp.float32)
    kappa = [full(cost_ref[i]) * (1.0 / (288.0 * spacing[i])) for i in range(5)]
    gain = [full(gain_ref[i]) * 12.0 / full(cost_ref[i]) for i in range(5)]
    base_b = 2 * rows * nx
    cos_a = lambda r: full(trig_ref[ix * rows + r])
    sin_a = lambda r: full(trig_ref[rows * nx + ix * rows + r])
    cos_b = lambda c: full(trig_ref[base_b + iy * cols + c])
    sin_b = lambda c: full(trig_ref[base_b + cols * ny + iy * cols + c])

    lane = lax.broadcasted_iota(jnp.int32, (8, LANES), 1)
    sublane = lax.broadcasted_iota(jnp.int32, (8, LANES), 0)
    x0 = ((sublane % planes).astype(jnp.float32) - planes / 2 + 0.5) * (2.0 / GRID)
    v[0:PAD, :] = jnp.zeros((PAD, LANES), jnp.float32)
    v[PAD + cells * block :, :] = jnp.zeros((PAD, LANES), jnp.float32)
    for k in range(parts):
        index = (k * pair + sublane // planes) * LANES + lane
        third, fourth = index // N4, index % N4
        x3 = (third.astype(jnp.float32) - N3 / 2 + 0.5) * (2.0 / GRID)
        x4 = (fourth.astype(jnp.float32) - N4 / 2 + 0.5) * (2.0 / GRID)
        f1[8 * k : 8 * k + 8, :] = gain[1] * (x4 - 0.3 * x0)
        f4k[8 * k : 8 * k + 8, :] = gain[4] * x4
        for r in range(rows):
            f2[8 * (r * parts + k) : 8 * (r * parts + k) + 8, :] = gain[2] * (x3 + 0.5 * sin_a(r))
        for slot, (spot, extent) in enumerate(((third, width // N4), (fourth, N4))):
            for i, off in enumerate((-3, -2, -1, 1, 2, 3)):
                good = (spot + off >= 0) & (spot + off < extent)
                first = 8 * ((slot * parts + k) * 6 + i)
                keep[first : first + 8, :] = jnp.where(good, 1.0, 0.0)
    for c in range(cols):
        f3[8 * c : 8 * c + 8, :] = gain[3] * (sin_b(c) - x0)
        for r in range(rows):
            i = c * rows + r
            f4r[8 * i : 8 * i + 8, :] = gain[4] * (cos_a(r) * sin_b(c))
    rowid = lax.broadcasted_iota(jnp.int32, (chunks, LANES), 0)
    laneid = lax.broadcasted_iota(jnp.int32, (chunks, LANES), 1)
    x3 = (((rowid * LANES + laneid) // N4).astype(jnp.float32) - N3 / 2 + 0.5) * (2.0 / GRID)
    for c in range(cols):
        for r in range(rows):
            i = c * rows + r
            bias = cos_a(r) - 0.5 * cos_b(c)
            f0[i * chunks : (i + 1) * chunks, :] = gain[0][0:1] * (bias[0:1] + x3)

    pl.semaphore_wait(barrier, n - 1)
    for c in range(cols):
        for copy in loads(c):
            copy.wait()
        for copy in sends(c):
            copy.start()

    zero = jnp.zeros((8, LANES), jnp.float32)

    def along_planes(g, top):
        def spot(p):
            return pl.ds(g * 8 * planes + p, 8, stride=planes)

        vs = [v[pl.ds(PAD + g * 8 * planes + p, 8, stride=planes), :] for p in range(planes)]
        drift = f0[span(g * 8), :]
        cellsp = wave(gaps([vs[0]] * 3 + vs + [vs[-1]] * 3))
        for p in range(planes):
            speed, part = tally(*cellsp[p], drift, kappa[0])
            top = jnp.maximum(top, speed)
            h[spot(p), :] = part
            q[0, spot(p), :] = cellsp[p][1]
        return top

    def along_lanes(slot, k, stride):
        number = 3 + slot

        def near(first, off):
            return v[pl.ds(first + off * planes, 8), :]

        def one(i, top):
            first = PAD + i * block + 8 * k
            vs = []
            for s in (-3, -2, -1, 0, 1, 2, 3):
                if s == 0:
                    vs.append(near(first, 0))
                    continue
                whole, rest = divmod(abs(s) * stride, LANES)
                if s > 0:
                    x = jnp.where(lane < rest, near(first, whole + 1), near(first, whole))
                    vs.append(pltpu.roll(x, LANES - rest, 1))
                else:
                    x = jnp.where(lane >= LANES - rest, near(first, -whole - 1), near(first, -whole))
                    vs.append(pltpu.roll(x, rest, 1))
            d = []
            for b in range(6):
                x = vs[b + 1] - vs[b]
                edge = slot == 1 or (k == 0 and b < 3) or (k == parts - 1 and b >= 3)
                if edge:
                    row = 8 * ((slot * parts + k) * 6 + b)
                    x = x * keep[row : row + 8, :]
                d.append(x)
            ((middle, jump),) = wave(d)
            if slot:
                drift = f4r[span(i * 8), :] - f4k[8 * k : 8 * k + 8, :]
            else:
                drift = f3[span(i // rows * 8), :]
            speed, part = tally(middle, jump, drift, kappa[number])
            here = span(i * block + 8 * k)
            q[number, here, :] = jump
            h[here, :] = h[here, :] + part
            return jnp.maximum(top, speed)

        def some(i, top):
            for u in range(3):
                top = one(i * 3 + u, top)
            return top

        return some

    def along_cols(i, top):
        r, k = i // parts, i % parts
        rim = [span((m * rows + r) * block + 8 * k) for m in range(3)]
        vs = [ca[x, :] for x in rim]
        vs += [v[span(PAD + (c * rows + r) * block + 8 * k), :] for c in range(cols)]
        vs += [cb[x, :] for x in rim]
        drift = f2[span(i * 8), :]
        for c, (middle, jump) in enumerate(wave(gaps(vs))):
            speed, part = tally(middle, jump, drift, kappa[2])
            top = jnp.maximum(top, speed)
            here = span((c * rows + r) * block + 8 * k)
            h[here, :] = h[here, :] + part
            q[2, here, :] = jump
        return top

    def along_rows(c, k, top):
        rim = [span((c * 3 + m) * block + 8 * k) for m in range(3)]
        vs = [ra[x, :] for x in rim]
        vs += [v[span(PAD + (c * rows + r) * block + 8 * k), :] for r in range(rows)]
        vs += [rb[x, :] for x in rim]
        drift = f1[span(k * 8), :]
        for r, (middle, jump) in enumerate(wave(gaps(vs))):
            speed, part = tally(middle, jump, drift, kappa[1])
            top = jnp.maximum(top, speed)
            here = span((c * rows + r) * block + 8 * k)
            h[here, :] = h[here, :] + part
            q[1, here, :] = jump
        return top

    def step(s, carry):
        tops = [None] * 5
        tops[0] = lax.fori_loop(0, cells * block // (8 * planes), along_planes, zero)
        for slot, stride in ((0, N4), (1, 1)):
            top = zero
            for k in range(parts):
                top = lax.fori_loop(0, cells // 3, along_lanes(slot, k, stride), top)
            tops[3 + slot] = top
        for c in range(3):
            for which in range(2):
                col_copy(c if which else c + cols - 3, which).wait()
        tops[2] = lax.fori_loop(0, rows * parts, along_cols, zero)
        row = lax.broadcasted_iota(jnp.int32, (8, LANES), 0)
        early = zero
        for number in (0, 2, 3, 4):
            early = jnp.where(row == number, jnp.max(tops[number]), early)
        top = zero
        for c in range(cols):
            for which in range(2):
                row_copy(c, which).wait()
            top = lax.fori_loop(0, parts, functools.partial(along_rows, c), top)
        own[...] = jnp.where(row == 1, jnp.max(top), early)

        def peak_copy(k):
            return pltpu.make_async_remote_copy(
                src_ref=own,
                dst_ref=slots.at[s, k],
                send_sem=ts_sem.at[k],
                recv_sem=tr_sem.at[s, k],
                device_id=place(k),
                device_id_type=MESH,
            )

        def send(k, carry):
            peak_copy(k).start()
            return carry

        def take(k, best):
            peak_copy(k).wait_recv()
            return jnp.maximum(best, slots[s, k])

        def finish(k, carry):
            peak_copy(k).wait_send()
            return carry

        lax.fori_loop(1, n, send, 0)
        best = lax.fori_loop(1, n, take, own[...])
        lax.fori_loop(1, n, finish, 0)
        spread = lambda i: jnp.broadcast_to(best[i : i + 1, :], (8, LANES))
        bounds = [spread(i) * full(cost_ref[i]) * (1.0 / 12.0) for i in range(5)]
        total = bounds[0] * (1.0 / spacing[0])
        for i in range(1, 5):
            total = total + bounds[i] * (1.0 / spacing[i])
        dt = COURANT / (total + 1e-6)
        scale = [dt * bounds[i] * (1.0 / (12.0 * spacing[i])) for i in range(5)]
        dt_ref[s] = dt[0, 0]

        @pl.when(s == 0)
        def _():
            for copy in masks():
                copy.wait()

        for c in range(cols):
            def move(i, carry):
                row = c * rows * block + i * 8
                here = span(row)
                change = dt * h[here, :]
                for number in range(5):
                    change = change - scale[number] * q[number, here, :]
                new = v[span(PAD + row), :] - change
                new = jnp.where(t[here, :] == 1, jnp.minimum(new, -0.5), new)
                v[span(PAD + row), :] = jnp.where(o[here, :] == 1, jnp.maximum(new, 0.5), new)
                return carry

            lax.fori_loop(0, rows * parts, move, 0, unroll=4)

            @pl.when(s < STEPS - 1)
            def _():
                for copy in sends(c):
                    copy.start()

            @pl.when(s == STEPS - 1)
            def _():
                for copy in stores(c):
                    copy.start()

        return carry

    lax.fori_loop(0, STEPS, step, 0)
    for c in range(cols):
        for copy in stores(c):
            copy.wait()


VMEM = pl.BlockSpec(memory_space=pltpu.VMEM)
SMEM = pl.BlockSpec(memory_space=pltpu.SMEM)
ANY = pl.BlockSpec(memory_space=pl.ANY)


def fold(x):
    planes, rows, cols, width = x.shape
    chunks = width // LANES
    x = x.reshape(planes, rows, cols, chunks, LANES).transpose(1, 2, 3, 0, 4)
    return x.reshape(rows * cols, chunks * planes, LANES)


def unfold(x, shape):
    planes, rows, cols, width = shape
    x = x.reshape(rows, cols, width // LANES, planes, LANES).transpose(3, 0, 1, 2, 4)
    return x.reshape(shape)


def body(value, target, obstacle, gains, costs):
    dims = value.shape
    planes, rows, cols, width = dims
    nx, ny = lax.axis_size("gx"), lax.axis_size("gy")
    block = planes * width // LANES
    parts = block // 8
    cells = rows * cols
    whole = cells * block
    one = np.float32(2.0 * math.pi / (rows * nx)) * np.arange(rows * nx, dtype=np.float32)
    two = np.float32(2.0 * math.pi / (cols * ny)) * np.arange(cols * ny, dtype=np.float32)
    one, two = one.astype(np.float64), two.astype(np.float64)
    trig = np.concatenate([np.cos(one), np.sin(one), np.cos(two), np.sin(two)])
    trig = jnp.asarray(trig.astype(np.float32))
    f32 = lambda *shape: pltpu.VMEM(shape, jnp.float32)
    i32 = lambda *shape: pltpu.VMEM(shape, jnp.int32)
    dma = lambda *shape: pltpu.SemaphoreType.DMA(shape)
    n = nx * ny
    out, steps = pl.pallas_call(
        functools.partial(kernel, dims, (nx, ny)),
        out_shape=[
            jax.ShapeDtypeStruct((cells, block, LANES), jnp.float32),
            jax.ShapeDtypeStruct((STEPS,), jnp.float32),
        ],
        in_specs=[SMEM, SMEM, SMEM, ANY, ANY, ANY],
        out_specs=[ANY, SMEM],
        scratch_shapes=[
            f32(whole + 2 * PAD, LANES), i32(whole, LANES), i32(whole, LANES),
            f32(whole, LANES), f32(5, whole, LANES),
            f32(cols * 3 * block, LANES), f32(cols * 3 * block, LANES),
            f32(rows * 3 * block, LANES), f32(rows * 3 * block, LANES),
            f32(whole // planes, LANES), f32(8 * parts, LANES), f32(8 * rows * parts, LANES),
            f32(8 * cols, LANES), f32(8 * cells, LANES), f32(8 * parts, LANES),
            f32(8 * 12 * parts, LANES), f32(8, LANES), f32(STEPS, n, 8, LANES),
            dma(3 * cells), dma(cells), dma(cols, 2), dma(cols, 2), dma(3, 2), dma(3, 2),
            dma(n), dma(STEPS, n),
        ],
        compiler_params=pltpu.CompilerParams(
            collective_id=0, has_side_effects=True, vmem_limit_bytes=40 << 20
        ),
    )(costs, gains, trig, fold(value), fold(target), fold(obstacle))
    return unfold(out, dims), steps


def solution(mesh):
    spec = P(None, "gx", "gy", None)
    return jax.shard_map(
        body,
        mesh=mesh,
        in_specs=(spec, spec, spec, P(), P()),
        out_specs=(spec, P()),
        check_vma=False,
    )
```

```python
import functools
import math

import jax
import jax.numpy as jnp
import numpy as np
from jax import lax
from jax.experimental.layout import Layout, with_layout_constraint
from jax.experimental import pallas as pl
from jax.experimental.pallas import tpu as pltpu
from jax.sharding import PartitionSpec as P

N3 = 32
N4 = 48
GRID = 96
STEPS = 3
COURANT = 0.5
EPS = 0.75e-6
LANES = 128
PAD = 16
UNROLL = 3
MESH = pl.DeviceIdType.MESH
DENSE = Layout(major_to_minor=(1, 2, 3, 0, 4))


def sub(x, y):
    if x is None or y is None:
        return x if y is None else -y
    return x - y


def add(x, y):
    if x is None or y is None:
        return x if y is None else y
    return x + y


def mul(x, y):
    return None if x is None or y is None else x * y


def wave(d):
    n = len(d) - 5
    f = [sub(d[k + 1], d[k]) for k in range(n + 4)]
    e = [sub(f[k + 1], f[k]) for k in range(n + 3)]
    j = [sub(e[k + 1], e[k]) for k in range(n + 2)]
    g = [mul(0.75, x) for x in f]
    g2 = [add(x, x) for x in g]
    base = [add(add(mul(e[k], e[k]), EPS), mul(g[k], f[k + 1])) for k in range(n + 3)]
    left, mid, right = [], [], []
    for k in range(n + 1):
        a = add(base[k], mul(g2[k + 1], e[k]))
        b = base[k + 1]
        c = sub(base[k + 2], mul(g2[k + 2], e[k + 2]))
        left.append(a * a)
        mid.append(b * b)
        right.append(c * c)
    low, high = [], []
    for k in range(n + 1):
        bc = mid[k] * right[k]
        ab = left[k] * mid[k]
        ac = 6.0 * (left[k] * right[k])
        n1 = mul(bc, j[k])
        n2 = mul(ab, j[k + 1])
        if 0 < k < n:
            both = add(n1, n2)
            both = add(both, both)
            core = (bc + ab) + ac
            low.append(add(both, n2) / (core + (ab + ab)))
            high.append(add(both, n1) / (core + (bc + bc)))
        elif k == 0:
            low.append(add(add(n1, n1), 3.0 * n2) / ((bc + ac) + 3.0 * ab))
            high.append(None)
        else:
            low.append(None)
            high.append(add(add(n2, n2), mul(3.0, n1)) / ((ab + ac) + 3.0 * bc))
    out = []
    for i in range(n):
        rm, rp = low[i], high[i + 1]
        center = mul(6.0, add(d[i + 3], d[i + 2]))
        middle = add(sub(center, add(e[i + 1], e[i + 2])), rp - rm)
        jump = sub(rp + rm, j[i + 1])
        out.append((middle, jump))
    return out


def gaps(vs):
    return [None if a is b else b - a for a, b in zip(vs[:-1], vs[1:])]


def tally(middle, jump, drift, kappa):
    gap = drift - middle
    return jnp.abs(gap) + jnp.abs(jump), (kappa * middle) * (drift + gap)


def kernel(
    dims, sizes,
    cost_hbm, gain_hbm, trig_hbm, v_hbm, t_hbm, o_hbm,
    out, dt_ref,
    v, t, o, h, q, ra, rb, ca, cb, f0, f1, f2, f3, f4r, f4k, keep, buf0, buf1, own, slots,
    in_sem, rs_sem, rr_sem, cs_sem, cr_sem, ts_sem, tr_sem, news,
    cost_ref, gain_ref, trig_ref, small_sem,
):
    planes, rows, cols, width = dims
    nx, ny = sizes
    chunks = width // LANES
    block = planes * chunks
    parts = block // 8
    pair = 8 // planes
    cells = rows * cols
    groups = cells // UNROLL
    ix, iy = lax.axis_index("gx"), lax.axis_index("gy")
    n = nx * ny
    h1 = 2.0 * math.pi / (rows * nx)
    h2 = 2.0 * math.pi / (cols * ny)
    spacing = [2.0 / GRID, h1, h2, 2.0 / GRID, 2.0 / GRID]

    def span(start, size=8):
        return pl.ds(pl.multiple_of(start, 8), size)

    def loads(c):
        out = []
        for r in range(rows):
            out.append(
                pltpu.make_async_copy(
                    v_hbm.at[r * cols + c],
                    v.at[pl.ds(PAD + (c * rows + r) * block, block)],
                    in_sem.at[c * rows + r],
                )
            )
        return out

    def masks():
        out = []
        for slot, (src, dst) in enumerate(((t_hbm, t), (o_hbm, o))):
            for c in range(cols):
                for r in range(rows):
                    out.append(
                        pltpu.make_async_copy(
                            src.at[r * cols + c],
                            dst.at[pl.ds((c * rows + r) * block, block)],
                            in_sem.at[(slot + 1) * cells + c * rows + r],
                        )
                    )
        return out

    tall = 3 * block
    up = ((ix + 1) % nx, iy)
    down = ((ix + nx - 1) % nx, iy)
    after = (ix, (iy + 1) % ny)
    before = (ix, (iy + ny - 1) % ny)

    def row_copy(c, which):
        first = PAD + c * rows * block + (0 if which else (rows - 3) * block)
        return pltpu.make_async_remote_copy(
            src_ref=v.at[pl.ds(first, tall)],
            dst_ref=(rb if which else ra).at[pl.ds(c * tall, tall)],
            send_sem=rs_sem.at[c, which],
            recv_sem=rr_sem.at[c, which],
            device_id=down if which else up,
            device_id_type=MESH,
        )

    def col_copy(c, which):
        wide = rows * block
        i = c if which else c - (cols - 3)
        return pltpu.make_async_remote_copy(
            src_ref=v.at[pl.ds(PAD + c * wide, wide)],
            dst_ref=(cb if which else ca).at[pl.ds(i * wide, wide)],
            send_sem=cs_sem.at[i, which],
            recv_sem=cr_sem.at[i, which],
            device_id=before if which else after,
            device_id_type=MESH,
        )

    def col_copies(c):
        out = []
        if c < 3:
            out.append(col_copy(c, 1))
        if c >= cols - 3:
            out.append(col_copy(c, 0))
        return out

    def sends(c):
        return [row_copy(c, 0), row_copy(c, 1)] + col_copies(c)

    around = (up, down, after, before)
    barrier = pltpu.get_barrier_semaphore()
    for other in around:
        pl.semaphore_signal(barrier, inc=1, device_id=other, device_id_type=MESH)
    for c in range(cols):
        for copy in loads(c):
            copy.start()

    smalls = [
        pltpu.make_async_copy(src, dst, small_sem.at[i])
        for i, (src, dst) in enumerate(
            ((cost_hbm, cost_ref), (gain_hbm, gain_ref), (trig_hbm, trig_ref))
        )
    ]
    for copy in smalls:
        copy.start()
    pl.semaphore_wait(barrier, 4)
    for c in range(cols):
        for copy in loads(c):
            copy.wait()
        for copy in sends(c):
            copy.start()
    for copy in masks():
        copy.start()

    for copy in smalls:
        copy.wait()

    full = lambda x: jnp.full((8, LANES), x, jnp.float32)
    kappa = [full(cost_ref[i]) * (1.0 / (288.0 * spacing[i])) for i in range(5)]
    gain = [full(gain_ref[i]) * 12.0 / full(cost_ref[i]) for i in range(5)]
    base_b = 2 * rows * nx
    cos_a = lambda r: full(trig_ref[ix * rows + r])
    sin_a = lambda r: full(trig_ref[rows * nx + ix * rows + r])
    cos_b = lambda c: full(trig_ref[base_b + iy * cols + c])
    sin_b = lambda c: full(trig_ref[base_b + cols * ny + iy * cols + c])

    lane = lax.broadcasted_iota(jnp.int32, (8, LANES), 1)
    sublane = lax.broadcasted_iota(jnp.int32, (8, LANES), 0)
    x0 = ((sublane % planes).astype(jnp.float32) - planes / 2 + 0.5) * (2.0 / GRID)
    v[0:PAD, :] = jnp.zeros((PAD, LANES), jnp.float32)
    v[PAD + cells * block :, :] = jnp.zeros((PAD, LANES), jnp.float32)
    for k in range(parts):
        index = (k * pair + sublane // planes) * LANES + lane
        third, fourth = index // N4, index % N4
        x3 = (third.astype(jnp.float32) - N3 / 2 + 0.5) * (2.0 / GRID)
        x4 = (fourth.astype(jnp.float32) - N4 / 2 + 0.5) * (2.0 / GRID)
        f1[8 * k : 8 * k + 8, :] = gain[1] * (x4 - 0.3 * x0)
        f4k[8 * k : 8 * k + 8, :] = gain[4] * x4
        for r in range(rows):
            f2[8 * (r * parts + k) : 8 * (r * parts + k) + 8, :] = gain[2] * (x3 + 0.5 * sin_a(r))
        for slot, (spot, extent) in enumerate(((third, width // N4), (fourth, N4))):
            for i, off in enumerate((-3, -2, -1, 1, 2, 3)):
                good = (spot + off >= 0) & (spot + off < extent)
                first = 8 * ((slot * parts + k) * 6 + i)
                keep[first : first + 8, :] = jnp.where(good, 1.0, 0.0)
    for c in range(cols):
        for r in range(rows):
            i = c * rows + r
            f4r[8 * i : 8 * i + 8, :] = gain[4] * (cos_a(r) * sin_b(c))
            f3[8 * i : 8 * i + 8, :] = gain[3] * (sin_b(c) - x0)
    rowid = lax.broadcasted_iota(jnp.int32, (chunks, LANES), 0)
    laneid = lax.broadcasted_iota(jnp.int32, (chunks, LANES), 1)
    x3 = (((rowid * LANES + laneid) // N4).astype(jnp.float32) - N3 / 2 + 0.5) * (2.0 / GRID)
    for c in range(cols):
        for r in range(rows):
            i = c * rows + r
            bias = cos_a(r) - 0.5 * cos_b(c)
            f0[i * chunks : (i + 1) * chunks, :] = gain[0][0:1] * (bias[0:1] + x3)

    zero = jnp.zeros((8, LANES), jnp.float32)

    def along_planes(g, top):
        def spot(p):
            return pl.ds(g * 8 * planes + p, 8, stride=planes)

        vs = [v[pl.ds(PAD + g * 8 * planes + p, 8, stride=planes), :] for p in range(planes)]
        drift = f0[span(g * 8), :]
        cellsp = wave(gaps([vs[0]] * 3 + vs + [vs[-1]] * 3))
        for p in range(planes):
            speed, part = tally(*cellsp[p], drift, kappa[0])
            top = jnp.maximum(top, speed)
            h[spot(p), :] = part
            q[0, spot(p), :] = cellsp[p][1]
        return top

    def along_lanes(slot, k, stride):
        number = 3 + slot

        def near(first, off):
            return v[pl.ds(first + off * planes, 8), :]

        def spin(group, buf):
            for u in range(UNROLL):
                first = PAD + (group * UNROLL + u) * block + 8 * k
                for b, s in enumerate((-3, -2, -1, 1, 2, 3)):
                    whole, rest = divmod(abs(s) * stride, LANES)
                    if s > 0:
                        x = jnp.where(lane < rest, near(first, whole + 1), near(first, whole))
                        x = pltpu.roll(x, LANES - rest, 1)
                    else:
                        x = jnp.where(lane >= LANES - rest, near(first, -whole - 1), near(first, -whole))
                        x = pltpu.roll(x, rest, 1)
                    row = 8 * (u * 6 + b)
                    buf[row : row + 8, :] = x

        def one(i, u, buf, top):
            turned = [buf[8 * (u * 6 + b) : 8 * (u * 6 + b) + 8, :] for b in range(6)]
            vs = turned[:3] + [near(PAD + i * block + 8 * k, 0)] + turned[3:]
            d = []
            for b in range(6):
                x = vs[b + 1] - vs[b]
                edge = slot == 1 or (k == 0 and b < 3) or (k == parts - 1 and b >= 3)
                if edge:
                    row = 8 * ((slot * parts + k) * 6 + b)
                    x = x * keep[row : row + 8, :]
                d.append(x)
            ((middle, jump),) = wave(d)
            if slot:
                drift = f4r[span(i * 8), :] - f4k[8 * k : 8 * k + 8, :]
            else:
                drift = f3[span(i * 8), :]
            speed, part = tally(middle, jump, drift, kappa[number])
            here = span(i * block + 8 * k)
            q[number, here, :] = jump
            h[here, :] = h[here, :] + part
            return jnp.maximum(top, speed)

        def some(i, top):
            spin(2 * i + 1, buf1)
            for u in range(UNROLL):
                top = one(2 * i * UNROLL + u, u, buf0, top)
            spin((2 * i + 2) % groups, buf0)
            for u in range(UNROLL):
                top = one((2 * i + 1) * UNROLL + u, u, buf1, top)
            return top

        def run(top):
            spin(0, buf0)
            return lax.fori_loop(0, groups // 2, some, top)

        return run

    def along_cols(i, top):
        r, k = i // parts, i % parts
        rim = [span((m * rows + r) * block + 8 * k) for m in range(3)]
        vs = [ca[x, :] for x in rim]
        vs += [v[span(PAD + (c * rows + r) * block + 8 * k), :] for c in range(cols)]
        vs += [cb[x, :] for x in rim]
        drift = f2[span(i * 8), :]
        for c, (middle, jump) in enumerate(wave(gaps(vs))):
            speed, part = tally(middle, jump, drift, kappa[2])
            top = jnp.maximum(top, speed)
            here = span((c * rows + r) * block + 8 * k)
            h[here, :] = h[here, :] + part
            q[2, here, :] = jump
        return top

    def along_rows(c, k, top):
        rim = [span((c * 3 + m) * block + 8 * k) for m in range(3)]
        vs = [ra[x, :] for x in rim]
        vs += [v[span(PAD + (c * rows + r) * block + 8 * k), :] for r in range(rows)]
        vs += [rb[x, :] for x in rim]
        drift = f1[span(k * 8), :]
        for r, (middle, jump) in enumerate(wave(gaps(vs))):
            speed, part = tally(middle, jump, drift, kappa[1])
            top = jnp.maximum(top, speed)
            here = span((c * rows + r) * block + 8 * k)
            h[here, :] = h[here, :] + part
            q[1, here, :] = jump
        return top

    hops = [(after, before)] * (ny // 2 - 1) + [(up, down)] * (nx // 2)

    def tell(i):
        for other in hops[i]:
            pl.semaphore_signal(news.at[i], inc=1, device_id=other, device_id_type=MESH)

    def gossip(s, turn):
        each = -(-len(hops) // (2 * parts))
        todo = range(turn * each, min((turn + 1) * each, len(hops)))

        @pl.when(s == 0)
        def _():
            for i in todo:
                pl.semaphore_wait(news.at[i], 2)
                if i + 1 < len(hops):
                    tell(i + 1)

    tell(0)

    def step(s, carry):
        tops = [None] * 5
        tops[0] = lax.fori_loop(0, cells * block // (8 * planes), along_planes, zero)
        for slot, stride in ((0, N4), (1, 1)):
            top = zero
            for k in range(parts):
                top = along_lanes(slot, k, stride)(top)
                gossip(s, slot * parts + k)
            tops[3 + slot] = top
        for c in range(3):
            for which in range(2):
                col_copy(c if which else c + cols - 3, which).wait()
        tops[2] = lax.fori_loop(0, rows * parts, along_cols, zero)
        early = zero
        for number in (0, 2, 3, 4):
            early = jnp.where(lane == number, jnp.max(tops[number]), early)
        top = zero
        for c in range(cols):
            for which in range(2):
                row_copy(c, which).wait()
            top = lax.fori_loop(0, parts, functools.partial(along_rows, c), top)
        mine = jnp.where(lane == 1, jnp.max(top), early)
        own[...] = mine

        def peak_copy(k):
            other = ((ix + k // ny) % nx, (iy + k % ny) % ny)
            return pltpu.make_async_remote_copy(
                src_ref=own.at[pl.ds(0, 1)],
                dst_ref=slots.at[pl.ds(s * n + k, 1)],
                send_sem=ts_sem.at[k],
                recv_sem=tr_sem.at[s, k],
                device_id=other,
                device_id_type=MESH,
            )

        for k in range(1, n):
            peak_copy(k).start()
        slots[pl.ds(s * n, 1), :] = mine[0:1]
        for k in range(1, n):
            peak_copy(k).wait_recv()
        best = slots[span(s * n), :]
        for k in range(8, n, 8):
            best = jnp.maximum(best, slots[span(s * n + k), :])
        best = jnp.max(best, axis=0, keepdims=True)
        spread = lambda i: jnp.broadcast_to(best[:, i : i + 1], (8, LANES))
        bounds = [spread(i) * full(cost_ref[i]) * (1.0 / 12.0) for i in range(5)]
        total = bounds[0] * (1.0 / spacing[0])
        for i in range(1, 5):
            total = total + bounds[i] * (1.0 / spacing[i])
        dt = COURANT / (total + 1e-6)
        scale = [dt * bounds[i] * (1.0 / (12.0 * spacing[i])) for i in range(5)]
        dt_ref[s] = dt[0, 0]

        @pl.when(s == 0)
        def _():
            for copy in masks():
                copy.wait()

        def launch(c, half):
            @pl.when(s < STEPS - 1)
            def _():
                row_copy(c, 1 - half).start()
                if half:
                    for copy in col_copies(c):
                        copy.start()

        pending = None
        for c in range(cols):
            for half in range(2):
                start = (c * rows + half * rows // 2) * block

                def move(i, carry):
                    row = start + i * 8
                    here = span(row)
                    change = dt * h[here, :]
                    for number in range(5):
                        change = change - scale[number] * q[number, here, :]
                    new = v[span(PAD + row), :] - change
                    new = jnp.where(t[here, :] == 1, jnp.minimum(new, -0.5), new)
                    new = jnp.where(o[here, :] == 1, jnp.maximum(new, 0.5), new)
                    v[span(PAD + row), :] = new
                    out[half * rows // 2 * cols + c + i // parts * cols, span(i % parts * 8), :] = new
                    return carry

                lax.fori_loop(0, rows * parts // 2, move, 0, unroll=6)
                if pending is not None:
                    launch(*pending)
                pending = (c, half)
        launch(*pending)
        for k in range(1, n):
            peak_copy(k).wait_send()
        return carry

    lax.fori_loop(0, STEPS, step, 0)


VMEM = pl.BlockSpec(memory_space=pltpu.VMEM)
SMEM = pl.BlockSpec(memory_space=pltpu.SMEM)
HBM = pl.BlockSpec(memory_space=pltpu.HBM)


def fold(x):
    planes, rows, cols, width = x.shape
    chunks = width // LANES
    x = with_layout_constraint(x.reshape(planes, rows, cols, chunks, LANES), DENSE)
    x = x.transpose(1, 2, 3, 0, 4)
    return x.reshape(rows * cols, chunks * planes, LANES)


def unfold(x, shape):
    planes, rows, cols, width = shape
    x = x.reshape(rows, cols, width // LANES, planes, LANES).transpose(3, 0, 1, 2, 4)
    return with_layout_constraint(x, DENSE).reshape(shape)


def body(value, target, obstacle, gains, costs):
    dims = value.shape
    planes, rows, cols, width = dims
    nx, ny = lax.axis_size("gx"), lax.axis_size("gy")
    block = planes * width // LANES
    parts = block // 8
    cells = rows * cols
    whole = cells * block
    one = np.float32(2.0 * math.pi / (rows * nx)) * np.arange(rows * nx, dtype=np.float32)
    two = np.float32(2.0 * math.pi / (cols * ny)) * np.arange(cols * ny, dtype=np.float32)
    one, two = one.astype(np.float64), two.astype(np.float64)
    trig = np.concatenate([np.cos(one), np.sin(one), np.cos(two), np.sin(two)])
    trig = jnp.asarray(trig.astype(np.float32))
    f32 = lambda *shape: pltpu.VMEM(shape, jnp.float32)
    i32 = lambda *shape: pltpu.VMEM(shape, jnp.int32)
    dma = lambda *shape: pltpu.SemaphoreType.DMA(shape)
    n = nx * ny
    out, steps = pl.pallas_call(
        functools.partial(kernel, dims, (nx, ny)),
        out_shape=[
            jax.ShapeDtypeStruct((cells, block, LANES), jnp.float32),
            jax.ShapeDtypeStruct((STEPS,), jnp.float32),
        ],
        in_specs=[HBM] * 6,
        out_specs=[VMEM, SMEM],
        scratch_shapes=[
            f32(whole + 2 * PAD, LANES), i32(whole, LANES), i32(whole, LANES),
            f32(whole, LANES), f32(5, whole, LANES),
            f32(cols * 3 * block, LANES), f32(cols * 3 * block, LANES),
            f32(rows * 3 * block, LANES), f32(rows * 3 * block, LANES),
            f32(whole // planes, LANES), f32(8 * parts, LANES), f32(8 * rows * parts, LANES),
            f32(8 * cells, LANES), f32(8 * cells, LANES), f32(8 * parts, LANES),
            f32(8 * 12 * parts, LANES), f32(48 * UNROLL, LANES), f32(48 * UNROLL, LANES),
            f32(8, LANES), f32(STEPS * n, LANES),
            dma(3 * cells), dma(cols, 2), dma(cols, 2), dma(3, 2), dma(3, 2),
            dma(n), dma(STEPS, n),
            pltpu.SemaphoreType.REGULAR((max(ny // 2 - 1 + nx // 2, 1),)),
            pltpu.SMEM((5,), jnp.float32), pltpu.SMEM((5,), jnp.float32),
            pltpu.SMEM(trig.shape, jnp.float32), dma(3),
        ],
        compiler_params=pltpu.CompilerParams(
            collective_id=0, has_side_effects=True, vmem_limit_bytes=40 << 20
        ),
    )(*[
        pltpu.with_memory_space_constraint(x, pltpu.HBM)
        for x in (costs, gains, trig, *map(fold, (value, target, obstacle)))
    ])
    return unfold(out, dims), steps


def solution(mesh):
    spec = P(None, "gx", "gy", None)
    return jax.shard_map(
        body,
        mesh=mesh,
        in_specs=(spec, spec, spec, P(), P()),
        out_specs=(spec, P()),
        check_vma=False,
    )
```

```python
import functools
import math

import jax
import jax.numpy as jnp
import numpy as np
from jax import lax
from jax.experimental.layout import Layout, with_layout_constraint
from jax.experimental import pallas as pl
from jax.experimental.pallas import tpu as pltpu
from jax.sharding import PartitionSpec as P

N3 = 32
N4 = 48
GRID = 96
STEPS = 3
COURANT = 0.5
EPS = 0.75e-6
LANES = 128
PAD = 16
UNROLL = 3
MESH = pl.DeviceIdType.MESH
DENSE = Layout(major_to_minor=(1, 2, 3, 0, 4))


def sub(x, y):
    if x is None or y is None:
        return x if y is None else -y
    return x - y


def add(x, y):
    if x is None or y is None:
        return x if y is None else y
    return x + y


def mul(x, y):
    return None if x is None or y is None else x * y


def wave(d):
    n = len(d) - 5
    f = [sub(d[k + 1], d[k]) for k in range(n + 4)]
    e = [sub(f[k + 1], f[k]) for k in range(n + 3)]
    j = [sub(e[k + 1], e[k]) for k in range(n + 2)]
    g = [mul(0.75, x) for x in f]
    g2 = [add(x, x) for x in g]
    base = [add(add(mul(e[k], e[k]), EPS), mul(g[k], f[k + 1])) for k in range(n + 3)]
    left, mid, right = [], [], []
    for k in range(n + 1):
        a = add(base[k], mul(g2[k + 1], e[k]))
        b = base[k + 1]
        c = sub(base[k + 2], mul(g2[k + 2], e[k + 2]))
        left.append(a * a)
        mid.append(b * b)
        right.append(c * c)
    low, high = [], []
    for k in range(n + 1):
        bc = mid[k] * right[k]
        ab = left[k] * mid[k]
        ac = 6.0 * (left[k] * right[k])
        n1 = mul(bc, j[k])
        n2 = mul(ab, j[k + 1])
        if 0 < k < n:
            both = add(n1, n2)
            both = add(both, both)
            core = (bc + ab) + ac
            low.append(add(both, n2) / (core + (ab + ab)))
            high.append(add(both, n1) / (core + (bc + bc)))
        elif k == 0:
            low.append(add(add(n1, n1), 3.0 * n2) / ((bc + ac) + 3.0 * ab))
            high.append(None)
        else:
            low.append(None)
            high.append(add(add(n2, n2), mul(3.0, n1)) / ((ab + ac) + 3.0 * bc))
    out = []
    for i in range(n):
        rm, rp = low[i], high[i + 1]
        center = mul(6.0, add(d[i + 3], d[i + 2]))
        middle = add(sub(center, add(e[i + 1], e[i + 2])), rp - rm)
        jump = sub(rp + rm, j[i + 1])
        out.append((middle, jump))
    return out


def gaps(vs):
    return [None if a is b else b - a for a, b in zip(vs[:-1], vs[1:])]


def tally(middle, jump, drift, kappa):
    gap = drift - middle
    return jnp.abs(gap) + jnp.abs(jump), (kappa * middle) * (drift + gap)


def kernel(
    dims, sizes,
    cost_hbm, gain_hbm, trig_hbm, v_hbm, t_hbm, o_hbm,
    out, dt_ref,
    v, t, o, work, ra, rb, ca, cb, f0, f1, f2, f3, f4r, f4k, keep, buf0, buf1, own, slots,
    in_sem, rs_sem, rr_sem, cs_sem, cr_sem, ts_sem, tr_sem, news,
    cost_ref, gain_ref, trig_ref, small_sem,
):
    planes, rows, cols, width = dims
    nx, ny = sizes
    chunks = width // LANES
    block = planes * chunks
    parts = block // 8
    pair = 8 // planes
    cells = rows * cols
    groups = cells // UNROLL
    ix, iy = lax.axis_index("gx"), lax.axis_index("gy")
    n = nx * ny
    h1 = 2.0 * math.pi / (rows * nx)
    h2 = 2.0 * math.pi / (cols * ny)
    spacing = [2.0 / GRID, h1, h2, 2.0 / GRID, 2.0 / GRID]

    def span(start, size=8):
        return pl.ds(pl.multiple_of(start, 8), size)

    def loads(c):
        out = []
        for r in range(rows):
            out.append(
                pltpu.make_async_copy(
                    v_hbm.at[r * cols + c],
                    v.at[pl.ds(PAD + (c * rows + r) * block, block)],
                    in_sem.at[c * rows + r],
                )
            )
        return out

    def masks():
        out = []
        for slot, (src, dst) in enumerate(((t_hbm, t), (o_hbm, o))):
            for c in range(cols):
                for r in range(rows):
                    out.append(
                        pltpu.make_async_copy(
                            src.at[r * cols + c],
                            dst.at[pl.ds((c * rows + r) * block, block)],
                            in_sem.at[(slot + 1) * cells + c * rows + r],
                        )
                    )
        return out

    tall = 3 * block
    up = ((ix + 1) % nx, iy)
    down = ((ix + nx - 1) % nx, iy)
    after = (ix, (iy + 1) % ny)
    before = (ix, (iy + ny - 1) % ny)

    def row_copy(c, which):
        first = PAD + c * rows * block + (0 if which else (rows - 3) * block)
        return pltpu.make_async_remote_copy(
            src_ref=v.at[pl.ds(first, tall)],
            dst_ref=(rb if which else ra).at[pl.ds(c * tall, tall)],
            send_sem=rs_sem.at[c, which],
            recv_sem=rr_sem.at[c, which],
            device_id=down if which else up,
            device_id_type=MESH,
        )

    def col_copy(c, which):
        wide = rows * block
        i = c if which else c - (cols - 3)
        return pltpu.make_async_remote_copy(
            src_ref=v.at[pl.ds(PAD + c * wide, wide)],
            dst_ref=(cb if which else ca).at[pl.ds(i * wide, wide)],
            send_sem=cs_sem.at[i, which],
            recv_sem=cr_sem.at[i, which],
            device_id=before if which else after,
            device_id_type=MESH,
        )

    def col_copies(c):
        out = []
        if c < 3:
            out.append(col_copy(c, 1))
        if c >= cols - 3:
            out.append(col_copy(c, 0))
        return out

    def start_row(c, turn):
        for odd in range(2):

            @pl.when(ix % 2 == odd)
            def _():
                row_copy(c, 1 - (turn + odd) % 2).start()

    def start_cols(c):
        for copy in col_copies(c):
            copy.start()

    around = (up, down, after, before)
    barrier = pltpu.get_barrier_semaphore()
    for other in around:
        pl.semaphore_signal(barrier, inc=1, device_id=other, device_id_type=MESH)
    for c in range(cols):
        for copy in loads(c):
            copy.start()

    smalls = [
        pltpu.make_async_copy(src, dst, small_sem.at[i])
        for i, (src, dst) in enumerate(
            ((cost_hbm, cost_ref), (gain_hbm, gain_ref), (trig_hbm, trig_ref))
        )
    ]
    for copy in smalls:
        copy.start()
    pl.semaphore_wait(barrier, 4)
    for c in range(cols):
        for copy in loads(c):
            copy.wait()
        start_row(c, 0)
        start_row(c, 1)
        start_cols(c)
    for copy in masks():
        copy.start()

    for copy in smalls:
        copy.wait()

    full = lambda x: jnp.full((8, LANES), x, jnp.float32)
    kappa = [full(cost_ref[i]) * (1.0 / (288.0 * spacing[i])) for i in range(5)]
    gain = [full(gain_ref[i]) * 12.0 / full(cost_ref[i]) for i in range(5)]
    base_b = 2 * rows * nx
    cos_a = lambda r: full(trig_ref[ix * rows + r])
    sin_a = lambda r: full(trig_ref[rows * nx + ix * rows + r])
    cos_b = lambda c: full(trig_ref[base_b + iy * cols + c])
    sin_b = lambda c: full(trig_ref[base_b + cols * ny + iy * cols + c])

    lane = lax.broadcasted_iota(jnp.int32, (8, LANES), 1)
    sublane = lax.broadcasted_iota(jnp.int32, (8, LANES), 0)
    x0 = ((sublane % planes).astype(jnp.float32) - planes / 2 + 0.5) * (2.0 / GRID)
    v[0:PAD, :] = jnp.zeros((PAD, LANES), jnp.float32)
    v[PAD + cells * block :, :] = jnp.zeros((PAD, LANES), jnp.float32)
    for k in range(parts):
        index = (k * pair + sublane // planes) * LANES + lane
        third, fourth = index // N4, index % N4
        x3 = (third.astype(jnp.float32) - N3 / 2 + 0.5) * (2.0 / GRID)
        x4 = (fourth.astype(jnp.float32) - N4 / 2 + 0.5) * (2.0 / GRID)
        f1[8 * k : 8 * k + 8, :] = gain[1] * (x4 - 0.3 * x0)
        f4k[8 * k : 8 * k + 8, :] = gain[4] * x4
        for r in range(rows):
            f2[8 * (r * parts + k) : 8 * (r * parts + k) + 8, :] = gain[2] * (x3 + 0.5 * sin_a(r))
        for slot, (spot, extent) in enumerate(((third, width // N4), (fourth, N4))):
            for i, off in enumerate((-3, -2, -1, 1, 2, 3)):
                good = (spot + off >= 0) & (spot + off < extent)
                first = 8 * ((slot * parts + k) * 6 + i)
                keep[first : first + 8, :] = jnp.where(good, 1.0, 0.0)
    for c in range(cols):
        for r in range(rows):
            i = c * rows + r
            f4r[8 * i : 8 * i + 8, :] = gain[4] * (cos_a(r) * sin_b(c))
            f3[8 * i : 8 * i + 8, :] = gain[3] * (sin_b(c) - x0)
    rowid = lax.broadcasted_iota(jnp.int32, (chunks, LANES), 0)
    laneid = lax.broadcasted_iota(jnp.int32, (chunks, LANES), 1)
    x3 = (((rowid * LANES + laneid) // N4).astype(jnp.float32) - N3 / 2 + 0.5) * (2.0 / GRID)
    for c in range(cols):
        for r in range(rows):
            i = c * rows + r
            bias = cos_a(r) - 0.5 * cos_b(c)
            f0[i * chunks : (i + 1) * chunks, :] = gain[0][0:1] * (bias[0:1] + x3)

    zero = jnp.zeros((8, LANES), jnp.float32)

    def along_planes(g, top):
        def spot(p):
            return pl.ds(g * 8 * planes + p, 8, stride=planes)

        vs = [v[pl.ds(PAD + g * 8 * planes + p, 8, stride=planes), :] for p in range(planes)]
        drift = f0[span(g * 8), :]
        cellsp = wave(gaps([vs[0]] * 3 + vs + [vs[-1]] * 3))
        for p in range(planes):
            speed, part = tally(*cellsp[p], drift, kappa[0])
            top = jnp.maximum(top, speed)
            work[0, spot(p), :] = part
            work[1, spot(p), :] = cellsp[p][1]
        return top

    def along_lanes(slot, k, stride):
        number = 3 + slot

        def near(first, off):
            return v[pl.ds(first + off * planes, 8), :]

        def spin(group, buf):
            for u in range(UNROLL):
                first = PAD + (group * UNROLL + u) * block + 8 * k
                for b, s in enumerate((-3, -2, -1, 1, 2, 3)):
                    whole, rest = divmod(abs(s) * stride, LANES)
                    if s > 0:
                        x = jnp.where(lane < rest, near(first, whole + 1), near(first, whole))
                        x = pltpu.roll(x, LANES - rest, 1)
                    else:
                        x = jnp.where(lane >= LANES - rest, near(first, -whole - 1), near(first, -whole))
                        x = pltpu.roll(x, rest, 1)
                    row = 8 * (u * 6 + b)
                    buf[row : row + 8, :] = x

        def one(i, u, buf, top):
            turned = [buf[8 * (u * 6 + b) : 8 * (u * 6 + b) + 8, :] for b in range(6)]
            vs = turned[:3] + [near(PAD + i * block + 8 * k, 0)] + turned[3:]
            d = []
            for b in range(6):
                x = vs[b + 1] - vs[b]
                edge = slot == 1 or (k == 0 and b < 3) or (k == parts - 1 and b >= 3)
                if edge:
                    row = 8 * ((slot * parts + k) * 6 + b)
                    x = x * keep[row : row + 8, :]
                d.append(x)
            ((middle, jump),) = wave(d)
            if slot:
                drift = f4r[span(i * 8), :] - f4k[8 * k : 8 * k + 8, :]
            else:
                drift = f3[span(i * 8), :]
            speed, part = tally(middle, jump, drift, kappa[number])
            here = span(i * block + 8 * k)
            work[1 + number, here, :] = jump
            work[0, here, :] = work[0, here, :] + part
            return jnp.maximum(top, speed)

        def some(i, top):
            spin(2 * i + 1, buf1)
            for u in range(UNROLL):
                top = one(2 * i * UNROLL + u, u, buf0, top)
            spin((2 * i + 2) % groups, buf0)
            for u in range(UNROLL):
                top = one((2 * i + 1) * UNROLL + u, u, buf1, top)
            return top

        def run(top):
            spin(0, buf0)
            return lax.fori_loop(0, groups // 2, some, top)

        return run

    def along_cols(i, top):
        r, k = i // parts, i % parts
        rim = [span((m * rows + r) * block + 8 * k) for m in range(3)]
        vs = [ca[x, :] for x in rim]
        vs += [v[span(PAD + (c * rows + r) * block + 8 * k), :] for c in range(cols)]
        vs += [cb[x, :] for x in rim]
        drift = f2[span(i * 8), :]
        for c, (middle, jump) in enumerate(wave(gaps(vs))):
            speed, part = tally(middle, jump, drift, kappa[2])
            top = jnp.maximum(top, speed)
            here = span((c * rows + r) * block + 8 * k)
            work[0, here, :] = work[0, here, :] + part
            work[3, here, :] = jump
        return top

    def along_rows(c, k, top):
        rim = [span((c * 3 + m) * block + 8 * k) for m in range(3)]
        vs = [ra[x, :] for x in rim]
        vs += [v[span(PAD + (c * rows + r) * block + 8 * k), :] for r in range(rows)]
        vs += [rb[x, :] for x in rim]
        drift = f1[span(k * 8), :]
        for r, (middle, jump) in enumerate(wave(gaps(vs))):
            speed, part = tally(middle, jump, drift, kappa[1])
            top = jnp.maximum(top, speed)
            here = span((c * rows + r) * block + 8 * k)
            work[0, here, :] = work[0, here, :] + part
            work[2, here, :] = jump
        return top

    hops = [(after, before)] * (ny // 2 - 1) + [(up, down)] * (nx // 2)

    def tell(i):
        for other in hops[i]:
            pl.semaphore_signal(news.at[i], inc=1, device_id=other, device_id_type=MESH)

    def gossip(s, turn):
        each = -(-len(hops) // (2 * parts))
        todo = range(turn * each, min((turn + 1) * each, len(hops)))

        @pl.when(s == 0)
        def _():
            for i in todo:
                pl.semaphore_wait(news.at[i], 2)
                if i + 1 < len(hops):
                    tell(i + 1)

    tell(0)

    order = list(range(1, n))

    def step(s, carry):
        tops = [None] * 5
        tops[0] = lax.fori_loop(0, cells * block // (8 * planes), along_planes, zero)
        for slot, stride in ((0, N4), (1, 1)):
            top = zero
            for k in range(parts):
                top = along_lanes(slot, k, stride)(top)
                gossip(s, slot * parts + k)
            tops[3 + slot] = top
        @pl.when(s == 0)
        def _():
            for copy in masks():
                copy.wait()

            def bound(i, carry):
                here = span(i * 8)
                work[6, here, :] = jnp.where(t[here, :] == 1, -0.5, jnp.inf)
                work[7, here, :] = jnp.where(o[here, :] == 1, 0.5, -jnp.inf)
                return carry

            lax.fori_loop(0, cells * parts, bound, 0, unroll=4)

        for c in range(3):
            for which in range(2):
                col_copy(c if which else c + cols - 3, which).wait()
        tops[2] = lax.fori_loop(0, rows * parts, along_cols, zero)
        early = zero
        for number in (0, 2, 3, 4):
            early = jnp.where(lane == number, jnp.max(tops[number]), early)
        own[...] = early
        top = zero
        for c in range(cols):
            for which in range(2):
                row_copy(c, which).wait()
            top = lax.fori_loop(0, parts, functools.partial(along_rows, c), top)
        own[1:2, :] = jnp.max(top, axis=0, keepdims=True)

        def peak_copy(k):
            other = ((ix + k // ny) % nx, (iy + k % ny) % ny)
            return pltpu.make_async_remote_copy(
                src_ref=own.at[pl.ds(0, 2)],
                dst_ref=slots.at[pl.ds((s * n + k) * 2, 2)],
                send_sem=ts_sem.at[k],
                recv_sem=tr_sem.at[s, k],
                device_id=other,
                device_id_type=MESH,
            )

        for k in order:
            peak_copy(k).start()
        slots[pl.ds(s * n * 2, 2), :] = own[0:2, :]
        for k in order:
            peak_copy(k).wait_recv()
        best = slots[span(s * n * 2), :]
        for k in range(8, 2 * n, 8):
            best = jnp.maximum(best, slots[span(s * n * 2 + k), :])
        best = jnp.maximum(best, pltpu.roll(best, 4, 0))
        best = jnp.maximum(best, pltpu.roll(best, 2, 0))
        last = jnp.max(best[1:2], axis=1, keepdims=True)
        spread = lambda i: jnp.broadcast_to(last if i == 1 else best[0:1, i : i + 1], (8, LANES))
        bounds = [spread(i) * full(cost_ref[i]) * (1.0 / 12.0) for i in range(5)]
        total = bounds[0] * (1.0 / spacing[0])
        for i in range(1, 5):
            total = total + bounds[i] * (1.0 / spacing[i])
        dt = COURANT / (total + 1e-6)
        scale = [dt * bounds[i] * (1.0 / (12.0 * spacing[i])) for i in range(5)]
        dt_ref[s] = dt[0, 0]

        def moved(row):
            here = span(row)
            change = dt * work[0, here, :]
            for number in range(5):
                change = change - scale[number] * work[1 + number, here, :]
            new = v[span(PAD + row), :] - change
            return jnp.maximum(jnp.minimum(new, work[6, here, :]), work[7, here, :])

        @pl.when(s == STEPS - 1)
        def _():
            def close(i, carry):
                c, r = i // rows, i % rows
                for k in range(parts):
                    out[r * cols + c, 8 * k : 8 * k + 8, :] = moved(i * block + 8 * k)
                return carry

            lax.fori_loop(0, cells, close, 0)

        @pl.when(s < STEPS - 1)
        def _():
            advance(moved)

        for k in order:
            peak_copy(k).wait_send()
        return carry

    def launch(c, half):
        start_row(c, half)
        if half:
            start_cols(c)

    def advance(moved):
        pending = None
        for c in range(cols):
            for half in range(2):
                start = (c * rows + (half + ix) % 2 * (rows // 2)) * block

                def move(i, carry):
                    row = start + i * 8
                    v[span(PAD + row), :] = moved(row)
                    return carry

                lax.fori_loop(0, rows * parts // 2, move, 0, unroll=6)
                if pending is not None:
                    launch(*pending)
                pending = (c, half)
        launch(*pending)

    lax.fori_loop(0, STEPS, step, 0)


VMEM = pl.BlockSpec(memory_space=pltpu.VMEM)
SMEM = pl.BlockSpec(memory_space=pltpu.SMEM)
HBM = pl.BlockSpec(memory_space=pltpu.HBM)


def fold(x):
    planes, rows, cols, width = x.shape
    chunks = width // LANES
    x = with_layout_constraint(x.reshape(planes, rows, cols, chunks, LANES), DENSE)
    x = x.transpose(1, 2, 3, 0, 4)
    return x.reshape(rows * cols, chunks * planes, LANES)


def unfold(x, shape):
    planes, rows, cols, width = shape
    x = x.reshape(rows, cols, width // LANES, planes, LANES).transpose(3, 0, 1, 2, 4)
    return with_layout_constraint(x, DENSE).reshape(shape)


def body(value, target, obstacle, gains, costs):
    dims = value.shape
    planes, rows, cols, width = dims
    nx, ny = lax.axis_size("gx"), lax.axis_size("gy")
    block = planes * width // LANES
    parts = block // 8
    cells = rows * cols
    whole = cells * block
    one = np.float32(2.0 * math.pi / (rows * nx)) * np.arange(rows * nx, dtype=np.float32)
    two = np.float32(2.0 * math.pi / (cols * ny)) * np.arange(cols * ny, dtype=np.float32)
    one, two = one.astype(np.float64), two.astype(np.float64)
    trig = np.concatenate([np.cos(one), np.sin(one), np.cos(two), np.sin(two)])
    trig = jnp.asarray(trig.astype(np.float32))
    f32 = lambda *shape: pltpu.VMEM(shape, jnp.float32)
    i32 = lambda *shape: pltpu.VMEM(shape, jnp.int32)
    dma = lambda *shape: pltpu.SemaphoreType.DMA(shape)
    n = nx * ny
    out, steps = pl.pallas_call(
        functools.partial(kernel, dims, (nx, ny)),
        out_shape=[
            jax.ShapeDtypeStruct((cells, block, LANES), jnp.float32),
            jax.ShapeDtypeStruct((STEPS,), jnp.float32),
        ],
        in_specs=[HBM] * 6,
        out_specs=[VMEM, SMEM],
        scratch_shapes=[
            f32(whole + 2 * PAD, LANES), i32(whole, LANES), i32(whole, LANES),
            f32(8, whole + 8, LANES),
            f32(cols * 3 * block, LANES), f32(cols * 3 * block, LANES),
            f32(rows * 3 * block, LANES), f32(rows * 3 * block, LANES),
            f32(whole // planes, LANES), f32(8 * parts, LANES), f32(8 * rows * parts, LANES),
            f32(8 * cells, LANES), f32(8 * cells, LANES), f32(8 * parts, LANES),
            f32(8 * 12 * parts, LANES), f32(48 * UNROLL, LANES), f32(48 * UNROLL, LANES),
            f32(8, LANES), f32(STEPS * n * 2, LANES),
            dma(3 * cells), dma(cols, 2), dma(cols, 2), dma(3, 2), dma(3, 2),
            dma(n), dma(STEPS, n),
            pltpu.SemaphoreType.REGULAR((max(ny // 2 - 1 + nx // 2, 1),)),
            pltpu.SMEM((5,), jnp.float32), pltpu.SMEM((5,), jnp.float32),
            pltpu.SMEM(trig.shape, jnp.float32), dma(3),
        ],
        compiler_params=pltpu.CompilerParams(
            collective_id=0, has_side_effects=True, vmem_limit_bytes=40 << 20
        ),
    )(*[
        pltpu.with_memory_space_constraint(x, pltpu.HBM)
        for x in (costs, gains, trig, *map(fold, (value, target, obstacle)))
    ])
    return unfold(out, dims), steps


def solution(mesh):
    spec = P(None, "gx", "gy", None)
    return jax.shard_map(
        body,
        mesh=mesh,
        in_specs=(spec, spec, spec, P(), P()),
        out_specs=(spec, P()),
        check_vma=False,
    )
```

```python
import functools
import math

import jax
import jax.numpy as jnp
import numpy as np
from jax import lax
from jax.experimental.layout import Layout, with_layout_constraint
from jax.experimental import pallas as pl
from jax.experimental.pallas import tpu as pltpu
from jax.sharding import PartitionSpec as P

N3 = 32
N4 = 48
GRID = 96
STEPS = 3
COURANT = 0.5
EPS = 0.75e-6
LANES = 128
PAD = 16
UNROLL = 3
MESH = pl.DeviceIdType.MESH
DENSE = Layout(major_to_minor=(1, 2, 3, 0, 4))


def sub(x, y):
    if x is None or y is None:
        return x if y is None else -y
    return x - y


def add(x, y):
    if x is None or y is None:
        return x if y is None else y
    return x + y


def mul(x, y):
    return None if x is None or y is None else x * y


def wave(d):
    n = len(d) - 5
    f = [sub(d[k + 1], d[k]) for k in range(n + 4)]
    e = [sub(f[k + 1], f[k]) for k in range(n + 3)]
    j = [sub(e[k + 1], e[k]) for k in range(n + 2)]
    g = [mul(0.75, x) for x in f]
    g2 = [add(x, x) for x in g]
    base = [add(add(mul(e[k], e[k]), EPS), mul(g[k], f[k + 1])) for k in range(n + 3)]
    left, mid, right = [], [], []
    for k in range(n + 1):
        a = add(base[k], mul(g2[k + 1], e[k]))
        b = base[k + 1]
        c = sub(base[k + 2], mul(g2[k + 2], e[k + 2]))
        left.append(a * a)
        mid.append(b * b)
        right.append(c * c)
    low, high = [], []
    for k in range(n + 1):
        bc = mid[k] * right[k]
        ab = left[k] * mid[k]
        ac = 6.0 * (left[k] * right[k])
        n1 = mul(bc, j[k])
        n2 = mul(ab, j[k + 1])
        if 0 < k < n:
            both = add(n1, n2)
            both = add(both, both)
            core = (bc + ab) + ac
            low.append(add(both, n2) / (core + (ab + ab)))
            high.append(add(both, n1) / (core + (bc + bc)))
        elif k == 0:
            low.append(add(add(n1, n1), 3.0 * n2) / ((bc + ac) + 3.0 * ab))
            high.append(None)
        else:
            low.append(None)
            high.append(add(add(n2, n2), mul(3.0, n1)) / ((ab + ac) + 3.0 * bc))
    out = []
    for i in range(n):
        rm, rp = low[i], high[i + 1]
        center = mul(6.0, add(d[i + 3], d[i + 2]))
        middle = add(sub(center, add(e[i + 1], e[i + 2])), rp - rm)
        jump = sub(rp + rm, j[i + 1])
        out.append((middle, jump))
    return out


def gaps(vs):
    return [None if a is b else b - a for a, b in zip(vs[:-1], vs[1:])]


def tally(middle, jump, drift, kappa):
    gap = drift - middle
    return jnp.abs(gap) + jnp.abs(jump), (kappa * middle) * (drift + gap)


def kernel(
    dims, sizes,
    cost_hbm, gain_hbm, trig_hbm, v_hbm, t_hbm, o_hbm,
    out, dt_ref,
    v, t, o, work, ra, rb, ca, cb, f0, f1, f2, f3, f4r, f4k, keep, buf0, buf1, own, slots,
    in_sem, rs_sem, rr_sem, cs_sem, cr_sem, ts_sem, tr_sem, news,
    cost_ref, gain_ref, trig_ref, small_sem,
):
    planes, rows, cols, width = dims
    nx, ny = sizes
    chunks = width // LANES
    block = planes * chunks
    parts = block // 8
    pair = 8 // planes
    cells = rows * cols
    groups = cells // UNROLL
    ix, iy = lax.axis_index("gx"), lax.axis_index("gy")
    n = nx * ny
    h1 = 2.0 * math.pi / (rows * nx)
    h2 = 2.0 * math.pi / (cols * ny)
    spacing = [2.0 / GRID, h1, h2, 2.0 / GRID, 2.0 / GRID]

    def span(start, size=8):
        return pl.ds(pl.multiple_of(start, 8), size)

    def loads(c):
        out = []
        for r in range(rows):
            out.append(
                pltpu.make_async_copy(
                    v_hbm.at[r * cols + c],
                    v.at[pl.ds(PAD + (c * rows + r) * block, block)],
                    in_sem.at[c * rows + r],
                )
            )
        return out

    def masks():
        out = []
        for slot, (src, dst) in enumerate(((t_hbm, t), (o_hbm, o))):
            for c in range(cols):
                for r in range(rows):
                    out.append(
                        pltpu.make_async_copy(
                            src.at[r * cols + c],
                            dst.at[pl.ds((c * rows + r) * block, block)],
                            in_sem.at[(slot + 1) * cells + c * rows + r],
                        )
                    )
        return out

    tall = 3 * block
    up = ((ix + 1) % nx, iy)
    down = ((ix + nx - 1) % nx, iy)
    after = (ix, (iy + 1) % ny)
    before = (ix, (iy + ny - 1) % ny)

    def row_copy(c, which):
        first = PAD + c * rows * block + (0 if which else (rows - 3) * block)
        return pltpu.make_async_remote_copy(
            src_ref=v.at[pl.ds(first, tall)],
            dst_ref=(rb if which else ra).at[pl.ds(c * tall, tall)],
            send_sem=rs_sem.at[c, which],
            recv_sem=rr_sem.at[c, which],
            device_id=down if which else up,
            device_id_type=MESH,
        )

    def col_copy(c, which):
        wide = rows * block
        i = c if which else c - (cols - 3)
        return pltpu.make_async_remote_copy(
            src_ref=v.at[pl.ds(PAD + c * wide, wide)],
            dst_ref=(cb if which else ca).at[pl.ds(i * wide, wide)],
            send_sem=cs_sem.at[i, which],
            recv_sem=cr_sem.at[i, which],
            device_id=before if which else after,
            device_id_type=MESH,
        )

    def col_copies(c):
        out = []
        if c < 3:
            out.append(col_copy(c, 1))
        if c >= cols - 3:
            out.append(col_copy(c, 0))
        return out

    def start_row(c, turn):
        for odd in range(2):

            @pl.when(ix % 2 == odd)
            def _():
                row_copy(c, 1 - (turn + odd) % 2).start()

    def start_cols(c):
        for copy in col_copies(c):
            copy.start()

    around = (up, down, after, before)
    barrier = pltpu.get_barrier_semaphore()
    for other in around:
        pl.semaphore_signal(barrier, inc=1, device_id=other, device_id_type=MESH)
    for c in range(cols):
        for copy in loads(c):
            copy.start()

    smalls = [
        pltpu.make_async_copy(src, dst, small_sem.at[i])
        for i, (src, dst) in enumerate(
            ((cost_hbm, cost_ref), (gain_hbm, gain_ref), (trig_hbm, trig_ref))
        )
    ]
    for copy in smalls:
        copy.start()
    pl.semaphore_wait(barrier, 4)
    for c in range(cols):
        for copy in loads(c):
            copy.wait()
        start_row(c, 0)
        start_row(c, 1)
        start_cols(c)
    for copy in masks():
        copy.start()

    for copy in smalls:
        copy.wait()

    full = lambda x: jnp.full((8, LANES), x, jnp.float32)
    kappa = [full(cost_ref[i]) * (1.0 / (288.0 * spacing[i])) for i in range(5)]
    gain = [full(gain_ref[i]) * 12.0 / full(cost_ref[i]) for i in range(5)]
    base_b = 2 * rows * nx
    cos_a = lambda r: full(trig_ref[ix * rows + r])
    sin_a = lambda r: full(trig_ref[rows * nx + ix * rows + r])
    cos_b = lambda c: full(trig_ref[base_b + iy * cols + c])
    sin_b = lambda c: full(trig_ref[base_b + cols * ny + iy * cols + c])

    lane = lax.broadcasted_iota(jnp.int32, (8, LANES), 1)
    sublane = lax.broadcasted_iota(jnp.int32, (8, LANES), 0)
    x0 = ((sublane % planes).astype(jnp.float32) - planes / 2 + 0.5) * (2.0 / GRID)
    v[0:PAD, :] = jnp.zeros((PAD, LANES), jnp.float32)
    v[PAD + cells * block :, :] = jnp.zeros((PAD, LANES), jnp.float32)
    for k in range(parts):
        index = (k * pair + sublane // planes) * LANES + lane
        third, fourth = index // N4, index % N4
        x3 = (third.astype(jnp.float32) - N3 / 2 + 0.5) * (2.0 / GRID)
        x4 = (fourth.astype(jnp.float32) - N4 / 2 + 0.5) * (2.0 / GRID)
        f1[8 * k : 8 * k + 8, :] = gain[1] * (x4 - 0.3 * x0)
        f4k[8 * k : 8 * k + 8, :] = gain[4] * x4
        for r in range(rows):
            f2[8 * (r * parts + k) : 8 * (r * parts + k) + 8, :] = gain[2] * (x3 + 0.5 * sin_a(r))
        for slot, (spot, extent) in enumerate(((third, width // N4), (fourth, N4))):
            for i, off in enumerate((-3, -2, -1, 1, 2, 3)):
                good = (spot + off >= 0) & (spot + off < extent)
                first = 8 * ((slot * parts + k) * 6 + i)
                keep[first : first + 8, :] = jnp.where(good, 1.0, 0.0)
    for c in range(cols):
        for r in range(rows):
            i = c * rows + r
            f4r[8 * i : 8 * i + 8, :] = gain[4] * (cos_a(r) * sin_b(c))
            f3[8 * i : 8 * i + 8, :] = gain[3] * (sin_b(c) - x0)
    rowid = lax.broadcasted_iota(jnp.int32, (chunks, LANES), 0)
    laneid = lax.broadcasted_iota(jnp.int32, (chunks, LANES), 1)
    x3 = (((rowid * LANES + laneid) // N4).astype(jnp.float32) - N3 / 2 + 0.5) * (2.0 / GRID)
    for c in range(cols):
        for r in range(rows):
            i = c * rows + r
            bias = cos_a(r) - 0.5 * cos_b(c)
            f0[i * chunks : (i + 1) * chunks, :] = gain[0][0:1] * (bias[0:1] + x3)

    zero = jnp.zeros((8, LANES), jnp.float32)

    def along_planes(g, top):
        def spot(p):
            return pl.ds(g * 8 * planes + p, 8, stride=planes)

        vs = [v[pl.ds(PAD + g * 8 * planes + p, 8, stride=planes), :] for p in range(planes)]
        drift = f0[span(g * 8), :]
        cellsp = wave(gaps([vs[0]] * 3 + vs + [vs[-1]] * 3))
        for p in range(planes):
            speed, part = tally(*cellsp[p], drift, kappa[0])
            top = jnp.maximum(top, speed)
            work[0, spot(p), :] = part
            work[1, spot(p), :] = cellsp[p][1]
        return top

    def along_lanes(slot, k, stride):
        number = 3 + slot

        def near(first, off):
            return v[pl.ds(first + off * planes, 8), :]

        def spin(group, buf):
            for u in range(UNROLL):
                first = PAD + (group * UNROLL + u) * block + 8 * k
                for b, s in enumerate((-3, -2, -1, 1, 2, 3)):
                    whole, rest = divmod(abs(s) * stride, LANES)
                    if s > 0:
                        x = jnp.where(lane < rest, near(first, whole + 1), near(first, whole))
                        x = pltpu.roll(x, LANES - rest, 1)
                    else:
                        x = jnp.where(lane >= LANES - rest, near(first, -whole - 1), near(first, -whole))
                        x = pltpu.roll(x, rest, 1)
                    row = 8 * (u * 6 + b)
                    buf[row : row + 8, :] = x

        def one(i, u, buf, top):
            turned = [buf[8 * (u * 6 + b) : 8 * (u * 6 + b) + 8, :] for b in range(6)]
            vs = turned[:3] + [near(PAD + i * block + 8 * k, 0)] + turned[3:]
            d = []
            for b in range(6):
                x = vs[b + 1] - vs[b]
                edge = slot == 1 or (k == 0 and b < 3) or (k == parts - 1 and b >= 3)
                if edge:
                    row = 8 * ((slot * parts + k) * 6 + b)
                    x = x * keep[row : row + 8, :]
                d.append(x)
            ((middle, jump),) = wave(d)
            if slot:
                drift = f4r[span(i * 8), :] - f4k[8 * k : 8 * k + 8, :]
            else:
                drift = f3[span(i * 8), :]
            speed, part = tally(middle, jump, drift, kappa[number])
            here = span(i * block + 8 * k)
            work[1 + number, here, :] = jump
            work[0, here, :] = work[0, here, :] + part
            return jnp.maximum(top, speed)

        def some(i, top):
            spin(2 * i + 1, buf1)
            for u in range(UNROLL):
                top = one(2 * i * UNROLL + u, u, buf0, top)
            spin((2 * i + 2) % groups, buf0)
            for u in range(UNROLL):
                top = one((2 * i + 1) * UNROLL + u, u, buf1, top)
            return top

        def run(top):
            spin(0, buf0)
            return lax.fori_loop(0, groups // 2, some, top)

        return run

    def along_cols(i, top):
        r, k = i // parts, i % parts
        rim = [span((m * rows + r) * block + 8 * k) for m in range(3)]
        vs = [ca[x, :] for x in rim]
        vs += [v[span(PAD + (c * rows + r) * block + 8 * k), :] for c in range(cols)]
        vs += [cb[x, :] for x in rim]
        drift = f2[span(i * 8), :]
        for c, (middle, jump) in enumerate(wave(gaps(vs))):
            speed, part = tally(middle, jump, drift, kappa[2])
            top = jnp.maximum(top, speed)
            here = span((c * rows + r) * block + 8 * k)
            work[0, here, :] = work[0, here, :] + part
            work[3, here, :] = jump
        return top

    def along_rows(c, k, top):
        rim = [span((c * 3 + m) * block + 8 * k) for m in range(3)]
        vs = [ra[x, :] for x in rim]
        vs += [v[span(PAD + (c * rows + r) * block + 8 * k), :] for r in range(rows)]
        vs += [rb[x, :] for x in rim]
        drift = f1[span(k * 8), :]
        for r, (middle, jump) in enumerate(wave(gaps(vs))):
            speed, part = tally(middle, jump, drift, kappa[1])
            top = jnp.maximum(top, speed)
            here = span((c * rows + r) * block + 8 * k)
            work[0, here, :] = work[0, here, :] + part
            work[2, here, :] = jump
        return top

    hops = [(after, before)] * (ny // 2 - 1) + [(up, down)] * (nx // 2)

    def tell(i):
        for other in hops[i]:
            pl.semaphore_signal(news.at[i], inc=1, device_id=other, device_id_type=MESH)

    def gossip(s, turn):
        each = -(-len(hops) // (2 * parts))
        todo = range(turn * each, min((turn + 1) * each, len(hops)))

        @pl.when(s == 0)
        def _():
            for i in todo:
                pl.semaphore_wait(news.at[i], 2)
                if i + 1 < len(hops):
                    tell(i + 1)

    tell(0)

    order = list(range(1, n))

    def step(s, carry):
        tops = [None] * 5
        tops[0] = lax.fori_loop(0, cells * block // (8 * planes), along_planes, zero)
        for slot, stride in ((0, N4), (1, 1)):
            top = zero
            for k in range(parts):
                top = along_lanes(slot, k, stride)(top)
                gossip(s, slot * parts + k)
            tops[3 + slot] = top
        @pl.when(s == 0)
        def _():
            for copy in masks():
                copy.wait()

            def bound(i, carry):
                here = span(i * 8)
                work[6, here, :] = jnp.where(t[here, :] == 1, -0.5, jnp.inf)
                work[7, here, :] = jnp.where(o[here, :] == 1, 0.5, -jnp.inf)
                return carry

            lax.fori_loop(0, cells * parts, bound, 0, unroll=4)

        for c in range(3):
            for which in range(2):
                col_copy(c if which else c + cols - 3, which).wait()
        tops[2] = lax.fori_loop(0, rows * parts, along_cols, zero)
        early = zero
        for number in (0, 2, 3, 4):
            early = jnp.where(lane == number, jnp.max(tops[number]), early)
        own[...] = early
        top = zero
        for c in range(cols):
            for which in range(2):
                row_copy(c, which).wait()
            top = lax.fori_loop(0, parts, functools.partial(along_rows, c), top)
        own[1:2, :] = jnp.max(top, axis=0, keepdims=True)

        def peak_copy(k):
            other = ((ix + k // ny) % nx, (iy + k % ny) % ny)
            return pltpu.make_async_remote_copy(
                src_ref=own.at[pl.ds(0, 2)],
                dst_ref=slots.at[pl.ds((s * n + k) * 2, 2)],
                send_sem=ts_sem.at[k],
                recv_sem=tr_sem.at[s, k],
                device_id=other,
                device_id_type=MESH,
            )

        for k in order:
            peak_copy(k).start()
        slots[pl.ds(s * n * 2, 2), :] = own[0:2, :]
        for k in order:
            peak_copy(k).wait_recv()
        best = slots[span(s * n * 2), :]
        for k in range(8, 2 * n, 8):
            best = jnp.maximum(best, slots[span(s * n * 2 + k), :])
        best = jnp.maximum(best, pltpu.roll(best, 4, 0))
        best = jnp.maximum(best, pltpu.roll(best, 2, 0))
        last = jnp.max(best[1:2], axis=1, keepdims=True)
        spread = lambda i: jnp.broadcast_to(last if i == 1 else best[0:1, i : i + 1], (8, LANES))
        bounds = [spread(i) * full(cost_ref[i]) * (1.0 / 12.0) for i in range(5)]
        total = bounds[0] * (1.0 / spacing[0])
        for i in range(1, 5):
            total = total + bounds[i] * (1.0 / spacing[i])
        dt = COURANT / (total + 1e-6)
        scale = [dt * bounds[i] * (1.0 / (12.0 * spacing[i])) for i in range(5)]
        dt_ref[s] = dt[0, 0]

        def moved(row):
            here = span(row)
            change = dt * work[0, here, :]
            for number in range(5):
                change = change - scale[number] * work[1 + number, here, :]
            new = v[span(PAD + row), :] - change
            return jnp.maximum(jnp.minimum(new, work[6, here, :]), work[7, here, :])

        @pl.when(s == STEPS - 1)
        def _():
            def close(c, carry):
                for r in range(rows):
                    for k in range(parts):
                        row = (c * rows + r) * block + 8 * k
                        out[r * cols + c, 8 * k : 8 * k + 8, :] = moved(row)
                return carry

            lax.fori_loop(0, cols, close, 0)

        @pl.when(s < STEPS - 1)
        def _():
            advance(moved)

        for k in order:
            peak_copy(k).wait_send()
        return carry

    def launch(c, half):
        start_row(c, half)
        if half:
            start_cols(c)

    def advance(moved):
        pending = None
        for c in range(cols):
            for half in range(2):
                start = (c * rows + (half + ix) % 2 * (rows // 2)) * block

                def move(i, carry):
                    row = start + i * 8
                    v[span(PAD + row), :] = moved(row)
                    return carry

                lax.fori_loop(0, rows * parts // 2, move, 0, unroll=True)
                if pending is not None:
                    launch(*pending)
                pending = (c, half)
        launch(*pending)

    lax.fori_loop(0, STEPS, step, 0)


VMEM = pl.BlockSpec(memory_space=pltpu.VMEM)
SMEM = pl.BlockSpec(memory_space=pltpu.SMEM)
HBM = pl.BlockSpec(memory_space=pltpu.HBM)


def fold(x):
    planes, rows, cols, width = x.shape
    chunks = width // LANES
    x = with_layout_constraint(x.reshape(planes, rows, cols, chunks, LANES), DENSE)
    x = x.transpose(1, 2, 3, 0, 4)
    return x.reshape(rows * cols, chunks * planes, LANES)


def unfold(x, shape):
    planes, rows, cols, width = shape
    x = x.reshape(rows, cols, width // LANES, planes, LANES).transpose(3, 0, 1, 2, 4)
    return with_layout_constraint(x, DENSE).reshape(shape)


def body(value, target, obstacle, gains, costs):
    dims = value.shape
    planes, rows, cols, width = dims
    nx, ny = lax.axis_size("gx"), lax.axis_size("gy")
    block = planes * width // LANES
    parts = block // 8
    cells = rows * cols
    whole = cells * block
    one = np.float32(2.0 * math.pi / (rows * nx)) * np.arange(rows * nx, dtype=np.float32)
    two = np.float32(2.0 * math.pi / (cols * ny)) * np.arange(cols * ny, dtype=np.float32)
    one, two = one.astype(np.float64), two.astype(np.float64)
    trig = np.concatenate([np.cos(one), np.sin(one), np.cos(two), np.sin(two)])
    trig = jnp.asarray(trig.astype(np.float32))
    f32 = lambda *shape: pltpu.VMEM(shape, jnp.float32)
    i32 = lambda *shape: pltpu.VMEM(shape, jnp.int32)
    dma = lambda *shape: pltpu.SemaphoreType.DMA(shape)
    n = nx * ny
    out, steps = pl.pallas_call(
        functools.partial(kernel, dims, (nx, ny)),
        out_shape=[
            jax.ShapeDtypeStruct((cells, block, LANES), jnp.float32),
            jax.ShapeDtypeStruct((STEPS,), jnp.float32),
        ],
        in_specs=[HBM] * 6,
        out_specs=[VMEM, SMEM],
        scratch_shapes=[
            f32(whole + 2 * PAD, LANES), i32(whole, LANES), i32(whole, LANES),
            f32(8, whole + 8, LANES),
            f32(cols * 3 * block, LANES), f32(cols * 3 * block, LANES),
            f32(rows * 3 * block, LANES), f32(rows * 3 * block, LANES),
            f32(whole // planes, LANES), f32(8 * parts, LANES), f32(8 * rows * parts, LANES),
            f32(8 * cells, LANES), f32(8 * cells, LANES), f32(8 * parts, LANES),
            f32(8 * 12 * parts, LANES), f32(48 * UNROLL, LANES), f32(48 * UNROLL, LANES),
            f32(8, LANES), f32(STEPS * n * 2, LANES),
            dma(3 * cells), dma(cols, 2), dma(cols, 2), dma(3, 2), dma(3, 2),
            dma(n), dma(STEPS, n),
            pltpu.SemaphoreType.REGULAR((max(ny // 2 - 1 + nx // 2, 1),)),
            pltpu.SMEM((5,), jnp.float32), pltpu.SMEM((5,), jnp.float32),
            pltpu.SMEM(trig.shape, jnp.float32), dma(3),
        ],
        compiler_params=pltpu.CompilerParams(
            collective_id=0, has_side_effects=True, vmem_limit_bytes=40 << 20
        ),
    )(*[
        pltpu.with_memory_space_constraint(x, pltpu.HBM)
        for x in (costs, gains, trig, *map(fold, (value, target, obstacle)))
    ])
    return unfold(out, dims), steps


def solution(mesh):
    spec = P(None, "gx", "gy", None)
    return jax.shard_map(
        body,
        mesh=mesh,
        in_specs=(spec, spec, spec, P(), P()),
        out_specs=(spec, P()),
        check_vma=False,
    )
```
